256 devices in a mesh: blk: 64 (over z, y, x_hi), batch: 4 (over x_lo, core).
Axes of the slice: x: 4 (x_hi: 2, x_lo: 2; x = x_hi * 2 + x_lo), y: 4, z: 8, core: 2. Of those that a mesh axis runs over, the one named last changes fastest.
Arguments:
- coefficients: bfloat16 [120, 196608], P(None, ('blk', 'batch')), may hold values from -6 to 6
- transforms: bfloat16 [12, 24, 196608], P(None, 'batch', 'blk'), may hold values from -6 to 6
- basis: bfloat16 [120, 3, 32768], P(None, None, 'blk'), may hold values from -0.5 to 0.5
- template: bfloat16 [3, 32768], P(None, 'blk'), may hold values from -6 to 6
- skin_weights: bfloat16 [24, 32768], P(None, 'blk'), may hold values from 0.019897461 to 1
Outputs:
- skinned: bfloat16 [196608, 4, 3, 512], P(('blk', 'batch'))
The draws below stay inside these ranges and needn't reach their ends.
All inputs are finite; a program needn't handle non-finite values.
Results may differ from the reference program's by a relative error of at most 0.0049.
Values may be sent and summed in bfloat16 or wider, within the bound.
A program may use at most 192 MiB of HBM per device.

```python
import math
import jax
import jax.numpy as jnp
from jax import lax

K = 120
J = 24
VB = 512
R = 768
STEPS = 4
VERTS = 32768
CHARS = 196608
N_BLK = 64
N_BATCH = 4


def levels(stream_key, dims, pieces, low, top_value):
    def one(axis_at, parts):
        heights = jax.random.uniform(jax.random.fold_in(jax.random.fold_in(stream_key, 6), axis_at), (parts,), jnp.float32, low / len(pieces), top_value / len(pieces))
        return jnp.repeat(jnp.exp(heights), dims[axis_at] // parts).reshape((-1,) + (1,) * (len(dims) - axis_at - 1))

    gain = one(*pieces[0])
    for cut in pieces[1:]:
        gain = gain * one(*cut)
    return gain


def noise(rng, extent, spread, reach, pieces=(), held_as=jnp.bfloat16):
    entries = jax.random.normal(rng, extent, jnp.float32) * spread
    if len(pieces) > 0:
        entries = levels(rng, extent, pieces, -0.22, 0.18) * entries
    return jnp.clip(entries, min=-reach, max=reach).astype(held_as)


def setup_inputs(seed: int = 0) -> dict:
    keys = jax.random.split(jax.random.key(seed), 6)
    return {
        "coefficients": noise(keys[0], (K, CHARS), 1.0, 6.0, ((1, 256),)),
        "transforms": noise(keys[1], (12, J, CHARS), 1.0, 6.0, ((1, 4), (2, 64))),
        "basis": noise(keys[2], (K, 3, VERTS), K ** -0.5, 0.5, ((2, 64),)),
        "template": noise(keys[3], (3, VERTS), 1.0, 6.0, ((1, 64),)),
        "skin_weights": jnp.clip(jnp.exp(math.log(1.0) - 3.9171631 * jax.random.uniform(keys[4], (J, VERTS), jnp.float32) ** levels(keys[4], (J, VERTS), ((1, 64),), -0.2, 0.2)), 0.019897461, 1.0).astype(jnp.bfloat16),
    }


def skin_block(coefficients, joint_poses, basis_block, template_block, weight_block):
    flattened = basis_block.reshape(basis_block.shape[0], -1)
    shaped = jnp.dot(coefficients.T, flattened, preferred_element_type=jnp.float32)
    shaped = shaped + template_block.reshape(1, -1).astype(jnp.float32)
    shaped = shaped.reshape(coefficients.shape[1], 3, -1)
    blended = jnp.einsum("mjr,jv->mrv", joint_poses.astype(jnp.float32), weight_block.astype(jnp.float32))
    positions = []
    for matrix_row in range(3):
        component = blended[4 * matrix_row + 3]
        for column in range(3):
            component = component + blended[4 * matrix_row + column] * shaped[:, column, :]
        positions.append(component)
    return jnp.stack(positions, axis=1).astype(jnp.bfloat16)


def reference(coefficients, transforms, basis, template, skin_weights):
    weight_float = skin_weights.astype(jnp.float32)
    normalized = (weight_float / jnp.sum(weight_float, axis=0, keepdims=True)).astype(jnp.bfloat16)
    group_size = R * N_BATCH

    def per_group(cycle_group):
        offset = (cycle_group * group_size).astype(jnp.int32)
        group_coefficients = lax.dynamic_slice_in_dim(coefficients, offset, group_size, 1)
        group_poses = lax.dynamic_slice_in_dim(transforms, offset, group_size, 2)
        results = []
        for step_index in range(STEPS):
            block_index = jnp.mod(cycle_group - step_index, N_BLK).astype(jnp.int32)
            vertex_offset = (block_index * VB).astype(jnp.int32)
            basis_block = lax.dynamic_slice_in_dim(basis, vertex_offset, VB, 2)
            template_block = lax.dynamic_slice_in_dim(template, vertex_offset, VB, 1)
            weight_block = lax.dynamic_slice_in_dim(normalized, vertex_offset, VB, 1)
            results.append(skin_block(group_coefficients, group_poses, basis_block, template_block, weight_block))
        return jnp.stack(results, axis=1)

    stacked = lax.map(per_group, jnp.arange(N_BLK, dtype=jnp.int32))
    return stacked.reshape(N_BLK * group_size, STEPS, 3, VB)
```

```python
import functools

import jax
import jax.numpy as jnp
from jax import lax
from jax.experimental import pallas as pl
from jax.experimental.pallas import tpu as pltpu
from jax.sharding import PartitionSpec as P

MESH = pl.DeviceIdType.MESH
F32 = jnp.float32
BF16 = jnp.bfloat16
K, J, VB, R, STEPS = 120, 24, 512, 768, 4
CHUNK = 128
CHUNKS = R // CHUNK
HALF = VB // 2
PIECES = 5
ROW_GAP = 33


def gather_kernel(
    n_blk,
    coef_ref, tr_ref, bas_ref, tem_ref, wei_ref,
    y_ref, c_ref, w_ref, x_ref, tm_ref,
    got, weights, coef, norm, zs,
    t_send, t_recv, b_send, b_recv, f_send, f_recv, local,
):
    blk = lax.axis_index("blk")
    me = lax.axis_index("batch")
    core = lax.rem(me, 2)
    hi = me // 2
    odd = lax.rem(blk, 2)
    sibling = hi * 2 + (1 - core)
    across = (1 - hi) * 2 + core
    diagonal = (1 - hi) * 2 + (1 - core)
    peers = (sibling, across, diagonal)
    up = lax.rem(blk + 2, n_blk)
    down = lax.rem(blk + n_blk - 2, n_blk)
    beside = blk + 1 - 2 * odd
    half = pl.ds(pl.multiple_of(core * HALF, HALF), HALF)

    own = [
        pltpu.make_async_copy(tr_ref.at[:, :, pl.ds(pl.multiple_of(me * R, R), R)], got.at[0], local.at[0]),
        pltpu.make_async_copy(coef_ref, coef, local.at[1]),
        pltpu.make_async_copy(bas_ref, x_ref.at[0], local.at[2]),
        pltpu.make_async_copy(wei_ref, weights.at[0], local.at[3]),
        pltpu.make_async_copy(tem_ref, tm_ref.at[0], local.at[4]),
    ]
    for copy in own:
        copy.start()

    barrier = pltpu.get_barrier_semaphore()
    for target in (
        (blk, sibling), (blk, across), (blk, diagonal), (beside, across), (up, me), (down, me),
    ):
        pl.semaphore_signal(barrier, inc=1, device_id=target, device_id_type=MESH)
    pl.semaphore_wait(barrier, 6)

    def remote(src, dst, send, recv, target):
        return pltpu.make_async_remote_copy(
            src_ref=src, dst_ref=dst, send_sem=send, recv_sem=recv, device_id=target, device_id_type=MESH
        )

    def slot_parts(slot, span):
        return [x_ref.at[slot, e, :, span] for e in range(3)] + [
            weights.at[slot, :, span], tm_ref.at[slot, :, span],
        ]

    def own_parts(span):
        return [bas_ref.at[e, :, span] for e in range(3)] + [wei_ref.at[:, span], tem_ref.at[:, span]]

    first = [
        remote(s, d, b_send.at[0, p], b_recv.at[1, p], (beside, across))
        for p, (s, d) in enumerate(zip(own_parts(half), slot_parts(1, half)))
    ]
    upward = [
        remote(s, d, b_send.at[1, p], b_recv.at[2, p], (up, me))
        for p, (s, d) in enumerate(zip(own_parts(half), slot_parts(2, half)))
    ]
    third = 3 - 2 * odd
    sideways = [
        remote(s, d, b_send.at[2, p], b_recv.at[third, p], (beside, across))
        for p, (s, d) in enumerate(zip(slot_parts(2, half), slot_parts(third, half)))
    ]
    again = [
        remote(s, d, b_send.at[3, p], b_recv.at[3, p], (up, me))
        for p, (s, d) in enumerate(zip(slot_parts(1, half), slot_parts(3, half)))
    ]
    across_core = [
        [
            remote(s, s, f_send.at[slot - 1, p], f_recv.at[slot - 1, p], (blk, sibling))
            for p, s in enumerate(slot_parts(slot, half))
        ]
        for slot in (1, 2, 3)
    ]
    exchange = [
        remote(
            tr_ref.at[:, :, pl.ds(pl.multiple_of(peer * R, R), R)], got.at[r + 1],
            t_send.at[r], t_recv.at[r], (blk, peer),
        )
        for r, peer in enumerate(peers)
    ]
    for copy in exchange:
        copy.start()
    for copy in upward:
        copy.start()

    @pl.when(odd == 0)
    def _():
        for copy in first:
            copy.start()

    zs[...] = jnp.zeros_like(zs)
    norm[...] = jnp.zeros_like(norm)
    w_ref[...] = jnp.zeros_like(w_ref)
    own[1].wait()
    for at in range(CHUNKS):
        part = slice(at * CHUNK, (at + 1) * CHUNK)
        c_ref[part, :] = coef[:, part].astype(F32).T.astype(BF16)

    def spread(slot):
        raw = weights[slot].astype(F32)
        even = (raw / jnp.sum(raw, axis=0, keepdims=True)).astype(BF16).astype(F32)
        for g in range(4):
            norm[g * 8 : g * 8 + 6, :] = even[g * 6 : g * 6 + 6]
        rows = jnp.concatenate(
            [norm[pl.ds(pl.multiple_of(g * 8, 8), 8), :] for g in (me,) + peers], axis=0
        ).astype(BF16)
        for e in range(4):
            w_ref[slot, e, e * 32 : e * 32 + 32, :] = rows

    own[3].wait()
    spread(0)

    for p in range(PIECES):
        upward[p].wait_recv()
        sideways[p].start()
        across_core[1][p].start()
    for p in range(PIECES):
        first[p].wait_recv()
        across_core[0][p].start()

        @pl.when(odd == 0)
        def _(p=p):
            again[p].start()

    own[0].wait()
    for r in range(3):
        exchange[r].wait_recv()
    for m in range(12):
        for r in range(4):
            zs[m // 4, (m % 4) * 32 + r * 8 : (m % 4) * 32 + r * 8 + 6, :] = got[r, m].astype(F32)
    for at in range(CHUNKS):
        for d in range(3):
            y_ref[at, d] = zs[d, :, at * CHUNK : (at + 1) * CHUNK].T.astype(BF16)

    for p in range(PIECES):
        again[p].wait_recv()
        across_core[2][p].start()
    for slot in (1, 2, 3):
        for p in range(PIECES):
            across_core[slot - 1][p].wait_recv()
        spread(slot)

    for k in (2, 4):
        own[k].wait()
    for copy in exchange + upward + sideways + sum(across_core, []):
        copy.wait_send()

    @pl.when(odd == 0)
    def _():
        for copy in first + again:
            copy.wait_send()


def compute_kernel(y_ref, c_ref, w_ref, x_ref, tm_ref, o_ref, shaped, staged):
    at = pl.program_id(0)
    rows = pl.ds(pl.multiple_of(at * CHUNK, CHUNK), CHUNK)
    for s in range(STEPS):
        for vt in range(2):
            span = slice(vt * HALF, (vt + 1) * HALF)
            for e in range(3):
                shaped[vt, e] = jnp.dot(
                    c_ref[rows, :], x_ref[s, e, :, span], preferred_element_type=F32
                ) + tm_ref[s, e : e + 1, span].astype(F32)
            for d in range(3):
                pose = y_ref[at, d]
                total = jnp.dot(pose, w_ref[s, 3, :, span], preferred_element_type=F32)
                for e in range(3):
                    total = total + shaped[vt, e] * jnp.dot(
                        pose, w_ref[s, e, :, span], preferred_element_type=F32
                    )
                for h in range(2):
                    place = (vt * 2 + h) * STEPS + s
                    for c0 in range(0, CHUNK, 8):
                        staged[d, pl.ds(ROW_GAP * c0 + 2 * place, 8, stride=ROW_GAP), :] = total[
                            c0 : c0 + 8, h * 128 : (h + 1) * 128
                        ]
    for c in range(CHUNK):
        for d in range(3):
            low = staged[d, pl.ds(ROW_GAP * c, 8, stride=2), :]
            high = staged[d, pl.ds(ROW_GAP * c + 16, 8, stride=2), :]
            o_ref[c, d] = jnp.concatenate([low, high], axis=0).astype(BF16)


def per_device(n_blk, coefficients, transforms, basis, template, skin_weights):
    any_space = pl.BlockSpec(memory_space=pltpu.HBM)
    vmem = pl.BlockSpec(memory_space=pltpu.VMEM)
    shape = jax.ShapeDtypeStruct
    dma = pltpu.SemaphoreType.DMA
    gathered = pl.pallas_call(
        functools.partial(gather_kernel, n_blk),
        out_shape=[
            shape((CHUNKS, 3, CHUNK, 128), BF16),
            shape((R, K), BF16),
            shape((STEPS, 4, 128, VB), BF16),
            shape((STEPS, 3, K, VB), BF16),
            shape((STEPS, 3, VB), BF16),
        ],
        in_specs=[any_space] * 5,
        out_specs=[vmem] * 5,
        scratch_shapes=[
            pltpu.VMEM((4, 12, 6, R), BF16),
            pltpu.VMEM((STEPS, J, VB), BF16),
            pltpu.VMEM((K, R), BF16),
            pltpu.VMEM((32, VB), F32),
            pltpu.VMEM((3, 128, R), F32),
            dma((3,)), dma((3,)),
            dma((4, PIECES)), dma((4, PIECES)),
            dma((3, PIECES)), dma((3, PIECES)),
            dma((5,)),
        ],
        compiler_params=pltpu.CompilerParams(
            collective_id=0, has_side_effects=True, vmem_limit_bytes=24 * 2**20
        ),
        name="gather",
    )(coefficients, transforms, jnp.transpose(basis, (1, 0, 2)), template, skin_weights)
    posed = pl.pallas_call(
        compute_kernel,
        grid=(CHUNKS,),
        out_shape=shape((R, 3, 16, 128), BF16),
        in_specs=[vmem] * 5,
        out_specs=pl.BlockSpec((CHUNK, 3, 16, 128), lambda i: (i, 0, 0, 0)),
        scratch_shapes=[
            pltpu.VMEM((2, 3, CHUNK, HALF), F32),
            pltpu.VMEM((3, CHUNK * ROW_GAP + 8, 128), F32),
        ],
        compiler_params=pltpu.CompilerParams(vmem_limit_bytes=32 * 2**20),
        cost_estimate=pl.CostEstimate(flops=4 * 10**9, bytes_accessed=14 * 10**6, transcendentals=0),
        name="compute",
    )(*gathered)
    return posed.reshape(R, 3, 4, STEPS, 128).transpose(0, 3, 1, 2, 4).reshape(R, STEPS, 3, VB)


def solution(mesh):
    both = ("blk", "batch")
    return jax.shard_map(
        functools.partial(per_device, mesh.shape["blk"]),
        mesh=mesh,
        in_specs=(P(None, both), P(None, "batch", "blk"), P(None, None, "blk"), P(None, "blk"), P(None, "blk")),
        out_specs=P(both, None, None, None),
        check_vma=False,
    )
```

```python
import functools

import jax
import jax.numpy as jnp
from jax import lax
from jax.experimental import pallas as pl
from jax.experimental.pallas import tpu as pltpu
from jax.sharding import PartitionSpec as P

MESH = pl.DeviceIdType.MESH
F32 = jnp.float32
BF16 = jnp.bfloat16
K, J, VB, R, STEPS = 120, 24, 512, 768, 4
CHUNK = 128
CHUNKS = R // CHUNK
HALF = VB // 2
PIECES = 5
ROW_GAP = 17
STAGE_ROWS = CHUNK * ROW_GAP + 8
TURNS = 3
TURN = R // TURNS
PACKED = 2
GATHER_VMEM = 20 * 2**20
COMPUTE_VMEM = 20 * 2**20


def spread(raw, norm, groups, out_ref):
    raw = raw.astype(F32)
    even = (raw / jnp.sum(raw, axis=0, keepdims=True)).astype(BF16).astype(F32)
    for g in range(4):
        norm[g * 8 : g * 8 + 6, :] = even[g * 6 : g * 6 + 6]
    rows = jnp.concatenate([norm[pl.ds(pl.multiple_of(g * 8, 8), 8), :] for g in groups], axis=0).astype(BF16)
    for e in range(4):
        out_ref[e, e * 32 : e * 32 + 32, :] = rows


def shape_up(at, s, c_ref, x_ref, tm_ref, shaped):
    rows = pl.ds(pl.multiple_of(at * CHUNK, CHUNK), CHUNK)
    for vt in range(2):
        span = slice(vt * HALF, (vt + 1) * HALF)
        for e in range(3):
            shaped[vt, e] = jnp.dot(
                c_ref[rows, :], x_ref[s, e, :, span], preferred_element_type=F32
            ) + tm_ref[s, e : e + 1, span].astype(F32)


def pose(at, s, y_ref, w_ref, shaped, staged):
    for vt in range(2):
        span = slice(vt * HALF, (vt + 1) * HALF)
        for d in range(3):
            poses = y_ref[at, d]
            total = jnp.dot(poses, w_ref[3, :, span], preferred_element_type=F32)
            for e in range(3):
                total = total + shaped[vt, e] * jnp.dot(poses, w_ref[e, :, span], preferred_element_type=F32)
            for h in range(2):
                place = (vt * 2 + h) * STEPS + s
                for c0 in range(0, CHUNK, 8):
                    staged[d, pl.ds(ROW_GAP * c0 + place, 8, stride=ROW_GAP), :] = total[
                        c0 : c0 + 8, h * 128 : (h + 1) * 128
                    ]


def gather_kernel(
    n_blk,
    coef_ref, tr_ref, bas_ref, tem_ref, wei_ref,
    y_ref, c_ref, w_ref, x_ref, tm_ref, f_ref,
    got, weights, coef, norm, zs, w_now, shaped, shaped_own,
    t_send, t_recv, b_send, b_recv, f_send, f_recv, local,
):
    blk = lax.axis_index("blk")
    me = lax.axis_index("batch")
    core = lax.rem(me, 2)
    hi = me // 2
    odd = lax.rem(blk, 2)
    sibling = hi * 2 + (1 - core)
    across = (1 - hi) * 2 + core
    diagonal = (1 - hi) * 2 + (1 - core)
    peers = (sibling, across, diagonal)
    groups = (me,) + peers
    up = lax.rem(blk + 2, n_blk)
    down = lax.rem(blk + n_blk - 2, n_blk)
    beside = blk + 1 - 2 * odd
    half = pl.ds(pl.multiple_of(core * HALF, HALF), HALF)

    own = [
        pltpu.make_async_copy(coef_ref, coef, local.at[0]),
        pltpu.make_async_copy(bas_ref, x_ref.at[0], local.at[1]),
        pltpu.make_async_copy(wei_ref, weights.at[0], local.at[2]),
        pltpu.make_async_copy(tem_ref, tm_ref.at[0], local.at[3]),
    ]

    def turn_of(device, turn):
        return tr_ref.at[:, :, pl.ds(pl.multiple_of(device * R + turn * TURN, TURN), TURN)]

    kept = [pltpu.make_async_copy(turn_of(me, turn), got.at[turn, 0], local.at[4 + turn]) for turn in range(TURNS)]
    for copy in own + kept:
        copy.start()

    barrier = pltpu.get_barrier_semaphore()
    for target in ((blk, sibling), (blk, across), (blk, diagonal), (beside, across), (down, me)):
        pl.semaphore_signal(barrier, inc=1, device_id=target, device_id_type=MESH)
    pl.semaphore_wait(barrier, 5)

    def remote(src, dst, send, recv, target):
        return pltpu.make_async_remote_copy(
            src_ref=src, dst_ref=dst, send_sem=send, recv_sem=recv, device_id=target, device_id_type=MESH
        )

    def slot_parts(slot, span):
        return [weights.at[slot, :, span], tm_ref.at[slot, :, span]] + [
            x_ref.at[slot, e, :, span] for e in range(3)
        ]

    def own_parts(span):
        return [wei_ref.at[:, span], tem_ref.at[:, span]] + [bas_ref.at[e, :, span] for e in range(3)]

    first = [
        remote(s, d, b_send.at[0, p], b_recv.at[1, p], (beside, across))
        for p, (s, d) in enumerate(zip(own_parts(half), slot_parts(1, half)))
    ]
    upward = [
        remote(s, d, b_send.at[1, p], b_recv.at[2, p], (up, me))
        for p, (s, d) in enumerate(zip(own_parts(half), slot_parts(2, half)))
    ]
    third = 3 - 2 * odd
    sideways = [
        remote(s, d, b_send.at[2, p], b_recv.at[third, p], (beside, across))
        for p, (s, d) in enumerate(zip(slot_parts(2, half), slot_parts(third, half)))
    ]
    again = [
        remote(s, d, b_send.at[3, p], b_recv.at[3, p], (up, me))
        for p, (s, d) in enumerate(zip(slot_parts(1, half), slot_parts(3, half)))
    ]
    across_core = [
        [
            remote(s, s, f_send.at[slot - 1, p], f_recv.at[slot - 1, p], (blk, sibling))
            for p, s in enumerate(slot_parts(slot, half))
        ]
        for slot in (1, 2, 3)
    ]
    exchange = [
        [
            remote(turn_of(peer, turn), got.at[turn, r + 1], t_send.at[r, turn], t_recv.at[r, turn], (blk, peer))
            for r, peer in enumerate(peers)
        ]
        for turn in range(TURNS)
    ]
    for turn in range(TURNS):
        for copy in exchange[turn]:
            copy.start()
    for copy in upward:
        copy.start()

    @pl.when(odd == 0)
    def _():
        for copy in first:
            copy.start()

    zs[...] = jnp.zeros_like(zs)
    norm[...] = jnp.zeros_like(norm)
    w_now[...] = jnp.zeros_like(w_now)
    w_ref[...] = jnp.zeros_like(w_ref)
    own[0].wait()
    for at in range(CHUNKS):
        part = slice(at * CHUNK, (at + 1) * CHUNK)
        c_ref[part, :] = coef[:, part].astype(F32).T.astype(BF16)
    for k in (1, 2, 3):
        own[k].wait()
    spread(weights[0], norm, groups, w_now)

    parts = TURN // CHUNK
    for at in range(CHUNKS):
        shape_up(at, 0, c_ref, x_ref, tm_ref, shaped_own.at[at])

    def arrive(turn):
        kept[turn].wait()
        for copy in exchange[turn]:
            copy.wait_recv()
        for m in range(12):
            for r in range(4):
                row = (m % 4) * 32 + r * 8
                zs[m // 4, row : row + 6, :] = got[turn, r, m].astype(F32)
        for part in range(parts):
            for d in range(3):
                y_ref[turn * parts + part, d] = zs[d, :, part * CHUNK : (part + 1) * CHUNK].T.astype(BF16)

    def block(s, turn):
        for part in range(parts):
            at = turn * parts + part
            if s == 0:
                mine = shaped_own.at[at]
            else:
                mine = shaped.at[part]
                shape_up(at, s, c_ref, x_ref, tm_ref, mine)
            pose(at, s, y_ref, w_now, mine, f_ref.at[at])

    late = blk < 2

    def hand_slot_2(pieces):
        for p in pieces:
            upward[p].wait_recv()
            sideways[p].start()
            across_core[1][p].start()

    def hand_slot_1(pieces):
        for p in pieces:
            first[p].wait_recv()
            across_core[0][p].start()

            @pl.when(odd == 0)
            def _(p=p):
                again[p].start()

    def hand_slot_3(pieces):
        for p in pieces:
            again[p].wait_recv()
            across_core[2][p].start()

    arrive(0)
    block(0, 0)
    pl.when(jnp.logical_not(late))(lambda: hand_slot_2((0, 1, 2)))
    arrive(1)
    block(0, 1)
    pl.when(jnp.logical_not(late))(lambda: hand_slot_2((3, 4)))
    arrive(2)
    block(0, 2)
    pl.when(late)(lambda: hand_slot_2(range(PIECES)))

    for p in range(PIECES):
        across_core[1][p].wait_recv()
    spread(weights[2], norm, groups, w_now)
    block(2, 0)
    hand_slot_1((0, 1, 2, 3))
    block(2, 1)
    hand_slot_1((4,))
    block(2, 2)

    for p in range(PIECES):
        across_core[0][p].wait_recv()
    spread(weights[1], norm, groups, w_now)
    block(1, 0)
    block(1, 1)
    hand_slot_3((0, 1, 2))
    block(1, 2)
    hand_slot_3((3, 4))
    for p in range(PIECES):
        across_core[2][p].wait_recv()
    spread(weights[3], norm, groups, w_ref)

    for copy in sum(exchange, []) + upward + sideways + sum(across_core, []):
        copy.wait_send()

    @pl.when(odd == 0)
    def _():
        for copy in first + again:
            copy.wait_send()


def compute_kernel(y_ref, c_ref, w_ref, x_ref, tm_ref, _, o_ref, f_ref, *scratch):
    for part in range(PACKED):
        at = pl.program_id(0) * PACKED + part
        shaped = scratch[part]
        shape_up(at, 3, c_ref, x_ref, tm_ref, shaped)
        pose(at, 3, y_ref, w_ref, shaped, f_ref.at[at])
        for c in range(CHUNK):
            for d in range(3):
                o_ref[part * CHUNK + c, d] = f_ref[at, d, pl.ds(ROW_GAP * c, 16), :].astype(BF16)


def per_device(n_blk, coefficients, transforms, basis, template, skin_weights):
    hbm = pl.BlockSpec(memory_space=pltpu.HBM)
    vmem = pl.BlockSpec(memory_space=pltpu.VMEM)
    shape = jax.ShapeDtypeStruct
    dma = pltpu.SemaphoreType.DMA
    gathered = pl.pallas_call(
        functools.partial(gather_kernel, n_blk),
        out_shape=[
            shape((CHUNKS, 3, CHUNK, 128), BF16),
            shape((R, K), BF16),
            shape((4, 128, VB), BF16),
            shape((STEPS, 3, K, VB), BF16),
            shape((STEPS, 3, VB), BF16),
            shape((CHUNKS, 3, STAGE_ROWS, 128), F32),
        ],
        in_specs=[hbm] * 5,
        out_specs=[vmem] * 6,
        scratch_shapes=[
            pltpu.VMEM((TURNS, 4, 12, 6, TURN), BF16),
            pltpu.VMEM((STEPS, J, VB), BF16),
            pltpu.VMEM((K, R), BF16),
            pltpu.VMEM((32, VB), F32),
            pltpu.VMEM((3, 128, TURN), F32),
            pltpu.VMEM((4, 128, VB), BF16),
            pltpu.VMEM((TURN // CHUNK, 2, 3, CHUNK, HALF), F32),
            pltpu.VMEM((CHUNKS, 2, 3, CHUNK, HALF), F32),
            dma((3, TURNS)), dma((3, TURNS)),
            dma((4, PIECES)), dma((4, PIECES)),
            dma((3, PIECES)), dma((3, PIECES)),
            dma((4 + TURNS,)),
        ],
        compiler_params=pltpu.CompilerParams(
            collective_id=0, has_side_effects=True, vmem_limit_bytes=GATHER_VMEM
        ),
        cost_estimate=pl.CostEstimate(flops=3 * 10**9, bytes_accessed=2 * 10**6, transcendentals=0),
        name="gather",
    )(*(
        pltpu.with_memory_space_constraint(a, pltpu.HBM)
        for a in (coefficients, transforms, jnp.transpose(basis, (1, 0, 2)), template, skin_weights)
    ))
    posed, _ = pl.pallas_call(
        compute_kernel,
        grid=(CHUNKS // PACKED,),
        out_shape=[shape((R, 3, 16, 128), BF16), gathered[5]],
        input_output_aliases={5: 1},
        in_specs=[vmem] * 6,
        out_specs=[pl.BlockSpec((PACKED * CHUNK, 3, 16, 128), lambda i: (i, 0, 0, 0)), vmem],
        scratch_shapes=[
            pltpu.VMEM((2, 3, CHUNK, HALF), F32),
        ] * PACKED,
        compiler_params=pltpu.CompilerParams(vmem_limit_bytes=COMPUTE_VMEM),
        cost_estimate=pl.CostEstimate(flops=10**9, bytes_accessed=10**7, transcendentals=0),
        name="compute",
    )(*gathered)
    return posed.reshape(R, 3, 4, STEPS, 128).transpose(0, 3, 1, 2, 4).reshape(R, STEPS, 3, VB)


def solution(mesh):
    both = ("blk", "batch")
    return jax.shard_map(
        functools.partial(per_device, mesh.shape["blk"]),
        mesh=mesh,
        in_specs=(P(None, both), P(None, "batch", "blk"), P(None, None, "blk"), P(None, "blk"), P(None, "blk")),
        out_specs=P(both, None, None, None),
        check_vma=False,
    )
```

```python
import functools

import jax
import jax.numpy as jnp
from jax import lax
from jax.experimental import pallas as pl
from jax.experimental.pallas import tpu as pltpu
from jax.sharding import PartitionSpec as P

MESH = pl.DeviceIdType.MESH
F32 = jnp.float32
BF16 = jnp.bfloat16
K, J, VB, R, STEPS = 120, 24, 512, 768, 4
CHUNK = 128
CHUNKS = R // CHUNK
HALF = VB // 2
PIECES = 5
ROW_GAP = 17
STAGE_ROWS = CHUNK * ROW_GAP + 8
TURNS = 3
TURN = R // TURNS
PACKED = 2
GATHER_VMEM = 20 * 2**20
COMPUTE_VMEM = 20 * 2**20


def spread(raw, norm, groups, out_ref):
    raw = raw.astype(F32)
    even = (raw / jnp.sum(raw, axis=0, keepdims=True)).astype(BF16).astype(F32)
    for g in range(4):
        norm[g * 8 : g * 8 + 6, :] = even[g * 6 : g * 6 + 6]
    rows = jnp.concatenate([norm[pl.ds(pl.multiple_of(g * 8, 8), 8), :] for g in groups], axis=0).astype(BF16)
    for e in range(4):
        out_ref[e, e * 32 : e * 32 + 32, :] = rows


def shape_up(at, s, c_ref, x_ref, tm_ref, shaped):
    rows = pl.ds(pl.multiple_of(at * CHUNK, CHUNK), CHUNK)
    for vt in range(2):
        span = slice(vt * HALF, (vt + 1) * HALF)
        for e in range(3):
            shaped[vt, e] = jnp.dot(
                c_ref[rows, :], x_ref[s, e, :, span], preferred_element_type=F32
            ) + tm_ref[s, e : e + 1, span].astype(F32)


def pose(at, s, y_ref, w_ref, shaped, staged):
    for vt in range(2):
        span = slice(vt * HALF, (vt + 1) * HALF)
        for d in range(3):
            poses = y_ref[at, d]
            total = jnp.dot(poses, w_ref[3, :, span], preferred_element_type=F32)
            for e in range(3):
                total = total + shaped[vt, e] * jnp.dot(poses, w_ref[e, :, span], preferred_element_type=F32)
            for h in range(2):
                place = (vt * 2 + h) * STEPS + s
                for c0 in range(0, CHUNK, 8):
                    staged[d, pl.ds(ROW_GAP * c0 + place, 8, stride=ROW_GAP), :] = total[
                        c0 : c0 + 8, h * 128 : (h + 1) * 128
                    ]


def gather_kernel(
    n_blk,
    coef_ref, tr_ref, bas_ref, tem_ref, wei_ref,
    y_ref, c_ref, w_ref, x_ref, tm_ref, f_ref,
    got, weights, coef, norm, zs, w_now, shaped, shaped_own,
    t_send, t_recv, b_send, b_recv, f_send, f_recv, local,
):
    blk = lax.axis_index("blk")
    me = lax.axis_index("batch")
    core = lax.rem(me, 2)
    hi = me // 2
    odd = lax.rem(blk, 2)
    sibling = hi * 2 + (1 - core)
    across = (1 - hi) * 2 + core
    diagonal = (1 - hi) * 2 + (1 - core)
    peers = (sibling, across, diagonal)
    groups = (me,) + peers
    up = lax.rem(blk + 2, n_blk)
    down = lax.rem(blk + n_blk - 2, n_blk)
    beside = blk + 1 - 2 * odd
    half = pl.ds(pl.multiple_of(core * HALF, HALF), HALF)

    own = [
        pltpu.make_async_copy(coef_ref, coef, local.at[0]),
        pltpu.make_async_copy(bas_ref, x_ref.at[0], local.at[1]),
        pltpu.make_async_copy(wei_ref, weights.at[0], local.at[2]),
        pltpu.make_async_copy(tem_ref, tm_ref.at[0], local.at[3]),
    ]

    def turn_of(device, turn):
        return tr_ref.at[:, :, pl.ds(pl.multiple_of(device * R + turn * TURN, TURN), TURN)]

    kept = [pltpu.make_async_copy(turn_of(me, turn), got.at[turn, 0], local.at[4 + turn]) for turn in range(TURNS)]
    for copy in own + kept:
        copy.start()

    barrier = pltpu.get_barrier_semaphore()
    for target in ((blk, sibling), (blk, across), (blk, diagonal), (beside, across), (down, me)):
        pl.semaphore_signal(barrier, inc=1, device_id=target, device_id_type=MESH)
    pl.semaphore_wait(barrier, 5)

    def remote(src, dst, send, recv, target):
        return pltpu.make_async_remote_copy(
            src_ref=src, dst_ref=dst, send_sem=send, recv_sem=recv, device_id=target, device_id_type=MESH
        )

    def slot_parts(slot, span):
        return [weights.at[slot, :, span], tm_ref.at[slot, :, span]] + [
            x_ref.at[slot, e, :, span] for e in range(3)
        ]

    def own_parts(span):
        return [wei_ref.at[:, span], tem_ref.at[:, span]] + [bas_ref.at[e, :, span] for e in range(3)]

    first = [
        remote(s, d, b_send.at[0, p], b_recv.at[1, p], (beside, across))
        for p, (s, d) in enumerate(zip(own_parts(half), slot_parts(1, half)))
    ]
    upward = [
        remote(s, d, b_send.at[1, p], b_recv.at[2, p], (up, me))
        for p, (s, d) in enumerate(zip(own_parts(half), slot_parts(2, half)))
    ]
    third = 3 - 2 * odd
    sideways = [
        remote(s, d, b_send.at[2, p], b_recv.at[third, p], (beside, across))
        for p, (s, d) in enumerate(zip(slot_parts(2, half), slot_parts(third, half)))
    ]
    again = [
        remote(s, d, b_send.at[3, p], b_recv.at[3, p], (up, me))
        for p, (s, d) in enumerate(zip(slot_parts(1, half), slot_parts(3, half)))
    ]

    def across_core(slot, p):
        part = slot_parts(slot, half)[p]
        return remote(part, part, f_send.at[slot - 1, p], f_recv.at[slot - 1, p], (blk, sibling))

    exchange = [
        [
            remote(turn_of(peer, turn), got.at[turn, r + 1], t_send.at[r, turn], t_recv.at[r, turn], (blk, peer))
            for r, peer in enumerate(peers)
        ]
        for turn in range(TURNS)
    ]
    for turn in range(TURNS):
        for copy in exchange[turn]:
            copy.start()
    for copy in upward:
        copy.start()

    @pl.when(odd == 0)
    def _():
        for copy in first:
            copy.start()

    zs[...] = jnp.zeros_like(zs)
    norm[...] = jnp.zeros_like(norm)
    w_now[...] = jnp.zeros_like(w_now)
    w_ref[...] = jnp.zeros_like(w_ref)
    own[0].wait()
    for at in range(CHUNKS):
        part = slice(at * CHUNK, (at + 1) * CHUNK)
        c_ref[part, :] = coef[:, part].astype(F32).T.astype(BF16)
    for k in (1, 2, 3):
        own[k].wait()
    spread(weights[0], norm, groups, w_now)

    parts = TURN // CHUNK
    for at in range(CHUNKS):
        shape_up(at, 0, c_ref, x_ref, tm_ref, shaped_own.at[at])

    def arrive(turn):
        kept[turn].wait()
        for copy in exchange[turn]:
            copy.wait_recv()
        for m in range(12):
            for r in range(4):
                row = (m % 4) * 32 + r * 8
                zs[m // 4, row : row + 6, :] = got[turn, r, m].astype(F32)
        for part in range(parts):
            for d in range(3):
                y_ref[turn * parts + part, d] = zs[d, :, part * CHUNK : (part + 1) * CHUNK].T.astype(BF16)

    def block(s, turn):
        for part in range(parts):
            at = turn * parts + part
            if turn_is_own(s):
                mine = shaped_own.at[at]
            else:
                mine = shaped.at[part]
                shape_up(at, s, c_ref, x_ref, tm_ref, mine)
            pose(at, s, y_ref, w_now, mine, f_ref.at[at])

    def turn_is_own(s):
        return isinstance(s, int)

    even = odd == 0
    late = blk < 2
    prompt = jnp.logical_not(late)

    def hand_slot_2(pieces):
        for p in pieces:
            upward[p].wait_recv()
            sideways[p].start()
            across_core(2, p).start()

    def hand_slot_1(pieces):
        for p in pieces:
            first[p].wait_recv()
            across_core(1, p).start()

    def hand_slot_1_upward(pieces):
        for p in pieces:
            first[p].wait_recv()
            again[p].start()
            across_core(1, p).start()

    def hand_slot_3(pieces):
        for p in pieces:
            again[p].wait_recv()
            across_core(3, p).start()

    def where(condition, action, pieces):
        pl.when(condition)(lambda: action(pieces))

    every = range(PIECES)
    arrive(0)
    block(0, 0)
    where(prompt, hand_slot_2, (0, 1, 2))
    arrive(1)
    block(0, 1)
    where(prompt, hand_slot_2, (3, 4))
    where(odd == 1, hand_slot_1, every)
    arrive(2)
    block(0, 2)
    where(jnp.logical_and(late, even), hand_slot_2, every)

    one = 2 - odd
    for p in every:
        across_core(one, p).wait_recv()
    spread(weights[one], norm, groups, w_now)
    block(one, 0)
    where(even, hand_slot_1_upward, (0, 1, 2))
    block(one, 1)
    where(even, hand_slot_1_upward, (3, 4))
    where(jnp.logical_and(late, odd == 1), hand_slot_2, (0, 1, 2))
    block(one, 2)
    where(jnp.logical_and(late, odd == 1), hand_slot_2, (3, 4))

    two = 1 + odd
    for p in every:
        across_core(two, p).wait_recv()
    spread(weights[two], norm, groups, w_now)
    late_third = jnp.logical_and(even, blk < 4)
    block(two, 0)
    where(jnp.logical_and(odd == 1, prompt), hand_slot_3, every)
    block(two, 1)
    where(jnp.logical_and(even, blk >= 4), hand_slot_3, every)
    block(two, 2)
    where(jnp.logical_or(late, late_third), hand_slot_3, every)
    for p in every:
        across_core(3, p).wait_recv()
    spread(weights[3], norm, groups, w_ref)

    passed = [across_core(slot, p) for slot in (1, 2, 3) for p in every]
    for copy in sum(exchange, []) + upward + sideways + passed:
        copy.wait_send()

    @pl.when(odd == 0)
    def _():
        for copy in first + again:
            copy.wait_send()


def compute_kernel(y_ref, c_ref, w_ref, x_ref, tm_ref, _, o_ref, f_ref, *scratch):
    for part in range(PACKED):
        at = pl.program_id(0) * PACKED + part
        shaped = scratch[part]
        shape_up(at, 3, c_ref, x_ref, tm_ref, shaped)
        pose(at, 3, y_ref, w_ref, shaped, f_ref.at[at])
        for c in range(CHUNK):
            for d in range(3):
                o_ref[part * CHUNK + c, d] = f_ref[at, d, pl.ds(ROW_GAP * c, 16), :].astype(BF16)


def per_device(n_blk, coefficients, transforms, basis, template, skin_weights):
    hbm = pl.BlockSpec(memory_space=pltpu.HBM)
    vmem = pl.BlockSpec(memory_space=pltpu.VMEM)
    shape = jax.ShapeDtypeStruct
    dma = pltpu.SemaphoreType.DMA
    gathered = pl.pallas_call(
        functools.partial(gather_kernel, n_blk),
        out_shape=[
            shape((CHUNKS, 3, CHUNK, 128), BF16),
            shape((R, K), BF16),
            shape((4, 128, VB), BF16),
            shape((STEPS, 3, K, VB), BF16),
            shape((STEPS, 3, VB), BF16),
            shape((CHUNKS, 3, STAGE_ROWS, 128), F32),
        ],
        in_specs=[hbm] * 5,
        out_specs=[vmem] * 6,
        scratch_shapes=[
            pltpu.VMEM((TURNS, 4, 12, 6, TURN), BF16),
            pltpu.VMEM((STEPS, J, VB), BF16),
            pltpu.VMEM((K, R), BF16),
            pltpu.VMEM((32, VB), F32),
            pltpu.VMEM((3, 128, TURN), F32),
            pltpu.VMEM((4, 128, VB), BF16),
            pltpu.VMEM((TURN // CHUNK, 2, 3, CHUNK, HALF), F32),
            pltpu.VMEM((CHUNKS, 2, 3, CHUNK, HALF), F32),
            dma((3, TURNS)), dma((3, TURNS)),
            dma((4, PIECES)), dma((4, PIECES)),
            dma((3, PIECES)), dma((3, PIECES)),
            dma((4 + TURNS,)),
        ],
        compiler_params=pltpu.CompilerParams(
            collective_id=0, has_side_effects=True, vmem_limit_bytes=GATHER_VMEM
        ),
        cost_estimate=pl.CostEstimate(flops=3 * 10**9, bytes_accessed=2 * 10**6, transcendentals=0),
        name="gather",
    )(*(
        pltpu.with_memory_space_constraint(a, pltpu.HBM)
        for a in (coefficients, transforms, jnp.transpose(basis, (1, 0, 2)), template, skin_weights)
    ))
    posed, _ = pl.pallas_call(
        compute_kernel,
        grid=(CHUNKS // PACKED,),
        out_shape=[shape((R, 3, 16, 128), BF16), gathered[5]],
        input_output_aliases={5: 1},
        in_specs=[vmem] * 6,
        out_specs=[pl.BlockSpec((PACKED * CHUNK, 3, 16, 128), lambda i: (i, 0, 0, 0)), vmem],
        scratch_shapes=[
            pltpu.VMEM((2, 3, CHUNK, HALF), F32),
        ] * PACKED,
        compiler_params=pltpu.CompilerParams(vmem_limit_bytes=COMPUTE_VMEM),
        cost_estimate=pl.CostEstimate(flops=10**9, bytes_accessed=10**7, transcendentals=0),
        name="compute",
    )(*gathered)
    return posed.reshape(R, 3, 4, STEPS, 128).transpose(0, 3, 1, 2, 4).reshape(R, STEPS, 3, VB)


def solution(mesh):
    both = ("blk", "batch")
    return jax.shard_map(
        functools.partial(per_device, mesh.shape["blk"]),
        mesh=mesh,
        in_specs=(P(None, both), P(None, "batch", "blk"), P(None, None, "blk"), P(None, "blk"), P(None, "blk")),
        out_specs=P(both, None, None, None),
        check_vma=False,
    )
```

```python
import functools

import jax
import jax.numpy as jnp
from jax import lax
from jax.experimental import pallas as pl
from jax.experimental.pallas import tpu as pltpu
from jax.sharding import PartitionSpec as P

MESH = pl.DeviceIdType.MESH
F32 = jnp.float32
BF16 = jnp.bfloat16
K, J, VB, R, STEPS = 120, 24, 512, 768, 4
CHUNK = 128
CHUNKS = R // CHUNK
HALF = VB // 2
PIECES = 5
ROW_GAP = 17
STAGE_ROWS = CHUNK * ROW_GAP + 8
TURNS = 3
TURN = R // TURNS
PACKED = 2
GATHER_VMEM = 20 * 2**20
COMPUTE_VMEM = 20 * 2**20


def spread(raw, norm, groups, out_ref):
    raw = raw.astype(F32)
    even = (raw / jnp.sum(raw, axis=0, keepdims=True)).astype(BF16).astype(F32)
    for g in range(4):
        norm[g * 8 : g * 8 + 6, :] = even[g * 6 : g * 6 + 6]
    rows = jnp.concatenate([norm[pl.ds(pl.multiple_of(g * 8, 8), 8), :] for g in groups], axis=0).astype(BF16)
    for e in range(4):
        out_ref[e, e * 32 : e * 32 + 32, :] = rows


def shape_up(at, s, c_ref, x_ref, tm_ref, shaped):
    rows = pl.ds(pl.multiple_of(at * CHUNK, CHUNK), CHUNK)
    for vt in range(2):
        span = slice(vt * HALF, (vt + 1) * HALF)
        for e in range(3):
            shaped[vt, e] = jnp.dot(
                c_ref[rows, :], x_ref[s, e, :, span], preferred_element_type=F32
            ) + tm_ref[s, e : e + 1, span].astype(F32)


def pose(at, s, y_ref, w_ref, shaped, staged):
    for vt in range(2):
        span = slice(vt * HALF, (vt + 1) * HALF)
        for d in range(3):
            poses = y_ref[at, d]
            total = jnp.dot(poses, w_ref[3, :, span], preferred_element_type=F32)
            for e in range(3):
                total = total + shaped[vt, e] * jnp.dot(poses, w_ref[e, :, span], preferred_element_type=F32)
            for h in range(2):
                place = (vt * 2 + h) * STEPS + s
                for c0 in range(0, CHUNK, 8):
                    staged[d, pl.ds(ROW_GAP * c0 + place, 8, stride=ROW_GAP), :] = total[
                        c0 : c0 + 8, h * 128 : (h + 1) * 128
                    ]


def gather_kernel(
    n_blk,
    coef_ref, tr_ref, bas_ref, tem_ref, wei_ref,
    y_ref, c_ref, w_ref, x_ref, tm_ref, f_ref,
    got, weights, coef, norm, zs, w_now, shaped, shaped_own,
    t_send, t_recv, b_send, b_recv, f_send, f_recv, local,
):
    blk = lax.axis_index("blk")
    me = lax.axis_index("batch")
    core = lax.rem(me, 2)
    hi = me // 2
    odd = lax.rem(blk, 2)
    sibling = hi * 2 + (1 - core)
    across = (1 - hi) * 2 + core
    diagonal = (1 - hi) * 2 + (1 - core)
    peers = (sibling, across, diagonal)
    groups = (me,) + peers
    up = lax.rem(blk + 2, n_blk)
    down = lax.rem(blk + n_blk - 2, n_blk)
    beside = blk + 1 - 2 * odd
    ahead = lax.rem(blk + 1, n_blk)
    behind = lax.rem(blk + n_blk - 1, n_blk)
    to_first = ahead == 0
    from_last = blk == 0
    half = pl.ds(pl.multiple_of(core * HALF, HALF), HALF)

    own = [
        pltpu.make_async_copy(coef_ref, coef, local.at[0]),
        pltpu.make_async_copy(bas_ref, x_ref.at[0], local.at[1]),
        pltpu.make_async_copy(wei_ref, weights.at[0], local.at[2]),
        pltpu.make_async_copy(tem_ref, tm_ref.at[0], local.at[3]),
    ]

    def turn_of(device, turn):
        return tr_ref.at[:, :, pl.ds(pl.multiple_of(device * R + turn * TURN, TURN), TURN)]

    kept = [pltpu.make_async_copy(turn_of(me, turn), got.at[turn, 0], local.at[4 + turn]) for turn in range(TURNS)]
    for copy in own + kept:
        copy.start()

    barrier = pltpu.get_barrier_semaphore()
    for target in ((blk, sibling), (blk, across), (blk, diagonal), (beside, across), (down, me)):
        pl.semaphore_signal(barrier, inc=1, device_id=target, device_id_type=MESH)
    pl.when(from_last)(
        lambda: pl.semaphore_signal(barrier, inc=1, device_id=(behind, across), device_id_type=MESH)
    )
    pl.semaphore_wait(barrier, 5 + (blk + 1) // n_blk)

    def remote(src, dst, send, recv, target):
        return pltpu.make_async_remote_copy(
            src_ref=src, dst_ref=dst, send_sem=send, recv_sem=recv, device_id=target, device_id_type=MESH
        )

    def slot_parts(slot, span):
        return [weights.at[slot, :, span], tm_ref.at[slot, :, span]] + [
            x_ref.at[slot, e, :, span] for e in range(3)
        ]

    def own_parts(span):
        return [wei_ref.at[:, span], tem_ref.at[:, span]] + [bas_ref.at[e, :, span] for e in range(3)]

    first = [
        remote(s, d, b_send.at[0, p], b_recv.at[1, p], (beside, across))
        for p, (s, d) in enumerate(zip(own_parts(half), slot_parts(1, half)))
    ]
    upward = [
        remote(s, d, b_send.at[1, p], b_recv.at[2, p], (up, me))
        for p, (s, d) in enumerate(zip(own_parts(half), slot_parts(2, half)))
    ]
    third = 3 - 2 * odd
    sideways = [
        remote(s, d, b_send.at[2, p], b_recv.at[third, p], (beside, across))
        for p, (s, d) in enumerate(zip(slot_parts(2, half), slot_parts(third, half)))
    ]
    again = [
        remote(s, d, b_send.at[3, p], b_recv.at[3, p], (up, me))
        for p, (s, d) in enumerate(zip(slot_parts(1, half), slot_parts(3, half)))
    ]
    direct = [
        remote(s, d, b_send.at[0, p], b_recv.at[3, p], (ahead, across))
        for p, (s, d) in enumerate(zip(slot_parts(2, half), slot_parts(3, half)))
    ]

    def across_core(slot, p):
        part = slot_parts(slot, half)[p]
        return remote(part, part, f_send.at[slot - 1, p], f_recv.at[slot - 1, p], (blk, sibling))

    exchange = [
        [
            remote(turn_of(peer, turn), got.at[turn, r + 1], t_send.at[r, turn], t_recv.at[r, turn], (blk, peer))
            for r, peer in enumerate(peers)
        ]
        for turn in range(TURNS)
    ]
    for turn in range(TURNS):
        for copy in exchange[turn]:
            copy.start()
    for copy in upward:
        copy.start()

    @pl.when(odd == 0)
    def _():
        for copy in first:
            copy.start()

    zs[...] = jnp.zeros_like(zs)
    norm[...] = jnp.zeros_like(norm)
    w_now[...] = jnp.zeros_like(w_now)
    w_ref[...] = jnp.zeros_like(w_ref)
    own[0].wait()
    for at in range(CHUNKS):
        part = slice(at * CHUNK, (at + 1) * CHUNK)
        c_ref[part, :] = coef[:, part].astype(F32).T.astype(BF16)
    for k in (1, 2, 3):
        own[k].wait()
    spread(weights[0], norm, groups, w_now)

    parts = TURN // CHUNK
    for at in range(CHUNKS):
        shape_up(at, 0, c_ref, x_ref, tm_ref, shaped_own.at[at])

    def arrive(turn):
        kept[turn].wait()
        for copy in exchange[turn]:
            copy.wait_recv()
        for m in range(12):
            for r in range(4):
                row = (m % 4) * 32 + r * 8
                zs[m // 4, row : row + 6, :] = got[turn, r, m].astype(F32)
        for part in range(parts):
            for d in range(3):
                y_ref[turn * parts + part, d] = zs[d, :, part * CHUNK : (part + 1) * CHUNK].T.astype(BF16)

    def block(s, turn):
        for part in range(parts):
            at = turn * parts + part
            if turn_is_own(s):
                mine = shaped_own.at[at]
            else:
                mine = shaped.at[part]
                shape_up(at, s, c_ref, x_ref, tm_ref, mine)
            pose(at, s, y_ref, w_now, mine, f_ref.at[at])

    def turn_is_own(s):
        return isinstance(s, int)

    even = odd == 0
    late = blk < 2
    prompt = jnp.logical_not(late)

    def hand_slot_2(pieces):
        for p in pieces:
            upward[p].wait_recv()
            pl.when(to_first)(direct[p].start)
            sideways[p].start()
            across_core(2, p).start()

    def hand_slot_1(pieces):
        for p in pieces:
            first[p].wait_recv()
            across_core(1, p).start()

    def hand_slot_1_upward(pieces):
        for p in pieces:
            first[p].wait_recv()
            pl.when(up != 0)(again[p].start)
            across_core(1, p).start()

    def hand_slot_3(pieces):
        for p in pieces:
            again[p].wait_recv()
            across_core(3, p).start()

    def where(condition, action, pieces):
        pl.when(condition)(lambda: action(pieces))

    every = range(PIECES)
    arrive(0)
    block(0, 0)
    where(prompt, hand_slot_2, (0, 1, 2))
    arrive(1)
    block(0, 1)
    where(prompt, hand_slot_2, (3, 4))
    where(odd == 1, hand_slot_1, every)
    arrive(2)
    block(0, 2)
    where(jnp.logical_and(late, even), hand_slot_2, every)

    one = 2 - odd
    for p in every:
        across_core(one, p).wait_recv()
    spread(weights[one], norm, groups, w_now)
    block(one, 0)
    where(even, hand_slot_1_upward, (0, 1, 2))
    block(one, 1)
    where(even, hand_slot_1_upward, (3, 4))
    where(jnp.logical_and(late, odd == 1), hand_slot_2, every)
    block(one, 2)

    two = 1 + odd
    for p in every:
        across_core(two, p).wait_recv()
    spread(weights[two], norm, groups, w_now)
    last_third = jnp.logical_or(blk == 1, blk == 2)
    block(two, 0)
    where(jnp.logical_and(odd == 1, prompt), hand_slot_3, every)
    block(two, 1)
    where(jnp.logical_and(even, blk != 2), hand_slot_3, every)
    block(two, 2)
    where(last_third, hand_slot_3, every)
    for p in every:
        across_core(3, p).wait_recv()
    spread(weights[3], norm, groups, w_ref)

    passed = [across_core(slot, p) for slot in (1, 2, 3) for p in every]
    for copy in sum(exchange, []) + upward + sideways + passed:
        copy.wait_send()

    @pl.when(odd == 0)
    def _():
        for copy in first:
            copy.wait_send()

    @pl.when(jnp.logical_and(odd == 0, up != 0))
    def _():
        for copy in again:
            copy.wait_send()

    @pl.when(to_first)
    def _():
        for copy in direct:
            copy.wait_send()


def compute_kernel(y_ref, c_ref, w_ref, x_ref, tm_ref, _, o_ref, f_ref, *scratch):
    for part in range(PACKED):
        at = pl.program_id(0) * PACKED + part
        shaped = scratch[part]
        shape_up(at, 3, c_ref, x_ref, tm_ref, shaped)
        pose(at, 3, y_ref, w_ref, shaped, f_ref.at[at])
        for c in range(CHUNK):
            for d in range(3):
                o_ref[part * CHUNK + c, d] = f_ref[at, d, pl.ds(ROW_GAP * c, 16), :].astype(BF16)


def per_device(n_blk, coefficients, transforms, basis, template, skin_weights):
    hbm = pl.BlockSpec(memory_space=pltpu.HBM)
    vmem = pl.BlockSpec(memory_space=pltpu.VMEM)
    shape = jax.ShapeDtypeStruct
    dma = pltpu.SemaphoreType.DMA
    gathered = pl.pallas_call(
        functools.partial(gather_kernel, n_blk),
        out_shape=[
            shape((CHUNKS, 3, CHUNK, 128), BF16),
            shape((R, K), BF16),
            shape((4, 128, VB), BF16),
            shape((STEPS, 3, K, VB), BF16),
            shape((STEPS, 3, VB), BF16),
            shape((CHUNKS, 3, STAGE_ROWS, 128), F32),
        ],
        in_specs=[hbm] * 5,
        out_specs=[vmem] * 6,
        scratch_shapes=[
            pltpu.VMEM((TURNS, 4, 12, 6, TURN), BF16),
            pltpu.VMEM((STEPS, J, VB), BF16),
            pltpu.VMEM((K, R), BF16),
            pltpu.VMEM((32, VB), F32),
            pltpu.VMEM((3, 128, TURN), F32),
            pltpu.VMEM((4, 128, VB), BF16),
            pltpu.VMEM((TURN // CHUNK, 2, 3, CHUNK, HALF), F32),
            pltpu.VMEM((CHUNKS, 2, 3, CHUNK, HALF), F32),
            dma((3, TURNS)), dma((3, TURNS)),
            dma((4, PIECES)), dma((4, PIECES)),
            dma((3, PIECES)), dma((3, PIECES)),
            dma((4 + TURNS,)),
        ],
        compiler_params=pltpu.CompilerParams(
            collective_id=0, has_side_effects=True, vmem_limit_bytes=GATHER_VMEM
        ),
        cost_estimate=pl.CostEstimate(flops=3 * 10**9, bytes_accessed=2 * 10**6, transcendentals=0),
        name="gather",
    )(*(
        pltpu.with_memory_space_constraint(a, pltpu.HBM)
        for a in (coefficients, transforms, jnp.transpose(basis, (1, 0, 2)), template, skin_weights)
    ))
    posed, _ = pl.pallas_call(
        compute_kernel,
        grid=(CHUNKS // PACKED,),
        out_shape=[shape((R, 3, 16, 128), BF16), gathered[5]],
        input_output_aliases={5: 1},
        in_specs=[vmem] * 6,
        out_specs=[pl.BlockSpec((PACKED * CHUNK, 3, 16, 128), lambda i: (i, 0, 0, 0)), vmem],
        scratch_shapes=[
            pltpu.VMEM((2, 3, CHUNK, HALF), F32),
        ] * PACKED,
        compiler_params=pltpu.CompilerParams(vmem_limit_bytes=COMPUTE_VMEM),
        cost_estimate=pl.CostEstimate(flops=10**9, bytes_accessed=10**7, transcendentals=0),
        name="compute",
    )(*gathered)
    return posed.reshape(R, 3, 4, STEPS, 128).transpose(0, 3, 1, 2, 4).reshape(R, STEPS, 3, VB)


def solution(mesh):
    both = ("blk", "batch")
    return jax.shard_map(
        functools.partial(per_device, mesh.shape["blk"]),
        mesh=mesh,
        in_specs=(P(None, both), P(None, "batch", "blk"), P(None, None, "blk"), P(None, "blk"), P(None, "blk")),
        out_specs=P(both, None, None, None),
        check_vma=False,
    )
```

```python
import functools

import jax
import jax.numpy as jnp
from jax import lax
from jax.experimental import pallas as pl
from jax.experimental.pallas import tpu as pltpu
from jax.sharding import PartitionSpec as P

MESH = pl.DeviceIdType.MESH
F32 = jnp.float32
BF16 = jnp.bfloat16
K, J, VB, R, STEPS = 120, 24, 512, 768, 4
CHUNK = 128
CHUNKS = R // CHUNK
HALF = VB // 2
PIECES = 5
ROW_GAP = 17
STAGE_ROWS = CHUNK * ROW_GAP + 8
TURNS = 3
TURN = R // TURNS
PACKED = 2
GATHER_VMEM = 20 * 2**20
COMPUTE_VMEM = 20 * 2**20


def spread(raw, norm, groups, out_ref):
    raw = raw.astype(F32)
    even = (raw / jnp.sum(raw, axis=0, keepdims=True)).astype(BF16).astype(F32)
    for g in range(4):
        norm[g * 8 : g * 8 + 6, :] = even[g * 6 : g * 6 + 6]
    rows = jnp.concatenate([norm[pl.ds(pl.multiple_of(g * 8, 8), 8), :] for g in groups], axis=0).astype(BF16)
    for e in range(4):
        out_ref[e, e * 32 : e * 32 + 32, :] = rows


def shape_up(at, s, c_ref, x_ref, tm_ref, shaped):
    rows = pl.ds(pl.multiple_of(at * CHUNK, CHUNK), CHUNK)
    for vt in range(2):
        span = slice(vt * HALF, (vt + 1) * HALF)
        for e in range(3):
            shaped[vt, e] = jnp.dot(
                c_ref[rows, :], x_ref[s, e, :, span], preferred_element_type=F32
            ) + tm_ref[s, e : e + 1, span].astype(F32)


def pose(at, s, y_ref, w_ref, shaped, staged):
    for vt in range(2):
        span = slice(vt * HALF, (vt + 1) * HALF)
        for d in range(3):
            poses = y_ref[at, d]
            total = jnp.dot(poses, w_ref[3, :, span], preferred_element_type=F32)
            for e in range(3):
                total = total + shaped[vt, e] * jnp.dot(poses, w_ref[e, :, span], preferred_element_type=F32)
            for h in range(2):
                place = (vt * 2 + h) * STEPS + s
                for c0 in range(0, CHUNK, 8):
                    staged[d, pl.ds(ROW_GAP * c0 + place, 8, stride=ROW_GAP), :] = total[
                        c0 : c0 + 8, h * 128 : (h + 1) * 128
                    ]


def gather_kernel(
    n_blk,
    coef_ref, tr_ref, bas_ref, tem_ref, wei_ref,
    y_ref, c_ref, w_ref, x_ref, tm_ref, f_ref,
    got, weights, coef, norm, zs, w_now, shaped, shaped_own,
    t_send, t_recv, b_send, b_recv, f_send, f_recv, local,
):
    blk = lax.axis_index("blk")
    me = lax.axis_index("batch")
    core = lax.rem(me, 2)
    hi = me // 2
    odd = lax.rem(blk, 2)
    sibling = hi * 2 + (1 - core)
    across = (1 - hi) * 2 + core
    diagonal = (1 - hi) * 2 + (1 - core)
    peers = (sibling, across, diagonal)
    groups = (me,) + peers
    up = lax.rem(blk + 2, n_blk)
    down = lax.rem(blk + n_blk - 2, n_blk)
    beside = blk + 1 - 2 * odd
    ahead = lax.rem(blk + 1, n_blk)
    behind = lax.rem(blk + n_blk - 1, n_blk)
    to_first = ahead == 0
    from_last = blk == 0
    half = pl.ds(pl.multiple_of(core * HALF, HALF), HALF)

    own = [
        pltpu.make_async_copy(coef_ref, coef, local.at[0]),
        pltpu.make_async_copy(bas_ref, x_ref.at[0], local.at[1]),
        pltpu.make_async_copy(wei_ref, weights.at[0], local.at[2]),
        pltpu.make_async_copy(tem_ref, tm_ref.at[0], local.at[3]),
    ]

    def turn_of(device, turn):
        return tr_ref.at[:, :, pl.ds(pl.multiple_of(device * R + turn * TURN, TURN), TURN)]

    kept = [pltpu.make_async_copy(turn_of(me, turn), got.at[turn, 0], local.at[4 + turn]) for turn in range(TURNS)]
    for copy in own + kept:
        copy.start()

    barrier = pltpu.get_barrier_semaphore()
    for target in ((blk, sibling), (blk, across), (blk, diagonal), (beside, across), (down, me)):
        pl.semaphore_signal(barrier, inc=1, device_id=target, device_id_type=MESH)
    pl.when(from_last)(
        lambda: pl.semaphore_signal(barrier, inc=1, device_id=(behind, across), device_id_type=MESH)
    )
    pl.semaphore_wait(barrier, 5 + (blk + 1) // n_blk)

    def remote(src, dst, send, recv, target):
        return pltpu.make_async_remote_copy(
            src_ref=src, dst_ref=dst, send_sem=send, recv_sem=recv, device_id=target, device_id_type=MESH
        )

    def slot_parts(slot, span):
        return [weights.at[slot, :, span], tm_ref.at[slot, :, span]] + [
            x_ref.at[slot, e, :, span] for e in range(3)
        ]

    def own_parts(span):
        return [wei_ref.at[:, span], tem_ref.at[:, span]] + [bas_ref.at[e, :, span] for e in range(3)]

    first = [
        remote(s, d, b_send.at[0, p], b_recv.at[1, p], (beside, across))
        for p, (s, d) in enumerate(zip(own_parts(half), slot_parts(1, half)))
    ]
    upward = [
        remote(s, d, b_send.at[1, p], b_recv.at[2, p], (up, me))
        for p, (s, d) in enumerate(zip(own_parts(half), slot_parts(2, half)))
    ]
    third = 3 - 2 * odd
    sideways = [
        remote(s, d, b_send.at[2, p], b_recv.at[third, p], (beside, across))
        for p, (s, d) in enumerate(zip(slot_parts(2, half), slot_parts(third, half)))
    ]
    again = [
        remote(s, d, b_send.at[3, p], b_recv.at[3, p], (up, me))
        for p, (s, d) in enumerate(zip(slot_parts(1, half), slot_parts(3, half)))
    ]
    direct = [
        remote(s, d, b_send.at[0, p], b_recv.at[3, p], (ahead, across))
        for p, (s, d) in enumerate(zip(slot_parts(2, half), slot_parts(3, half)))
    ]

    def across_core(slot, p):
        part = slot_parts(slot, half)[p]
        return remote(part, part, f_send.at[slot - 1, p], f_recv.at[slot - 1, p], (blk, sibling))

    exchange = [
        [
            remote(turn_of(peer, turn), got.at[turn, r + 1], t_send.at[r, turn], t_recv.at[r, turn], (blk, peer))
            for r, peer in enumerate(peers)
        ]
        for turn in range(TURNS)
    ]
    for turn in range(TURNS):
        for copy in exchange[turn]:
            copy.start()
    for copy in upward:
        copy.start()

    @pl.when(odd == 0)
    def _():
        for copy in first:
            copy.start()

    zs[...] = jnp.zeros_like(zs)
    norm[...] = jnp.zeros_like(norm)
    w_now[...] = jnp.zeros_like(w_now)
    w_ref[...] = jnp.zeros_like(w_ref)
    own[0].wait()
    for at in range(CHUNKS):
        part = slice(at * CHUNK, (at + 1) * CHUNK)
        c_ref[part, :] = coef[:, part].astype(F32).T.astype(BF16)
    for k in (1, 2, 3):
        own[k].wait()
    spread(weights[0], norm, groups, w_now)

    parts = TURN // CHUNK
    for at in range(CHUNKS):
        shape_up(at, 0, c_ref, x_ref, tm_ref, shaped_own.at[at])

    def arrive(turn):
        kept[turn].wait()
        for copy in exchange[turn]:
            copy.wait_recv()
        for m in range(12):
            for r in range(4):
                row = (m % 4) * 32 + r * 8
                zs[m // 4, row : row + 6, :] = got[turn, r, m].astype(F32)
        for part in range(parts):
            for d in range(3):
                y_ref[turn * parts + part, d] = zs[d, :, part * CHUNK : (part + 1) * CHUNK].T.astype(BF16)

    def block(s, turn):
        for part in range(parts):
            at = turn * parts + part
            if turn_is_own(s):
                mine = shaped_own.at[at]
            else:
                mine = shaped.at[part]
                shape_up(at, s, c_ref, x_ref, tm_ref, mine)
            pose(at, s, y_ref, w_now, mine, f_ref.at[at])

    def turn_is_own(s):
        return isinstance(s, int)

    even = odd == 0
    late = blk < 2
    prompt = jnp.logical_not(late)

    def hand_slot_2(pieces):
        for p in pieces:
            upward[p].wait_recv()
            pl.when(to_first)(direct[p].start)
            sideways[p].start()
            across_core(2, p).start()

    def hand_slot_1(pieces):
        for p in pieces:
            first[p].wait_recv()
            across_core(1, p).start()

    def hand_slot_1_upward(pieces):
        for p in pieces:
            first[p].wait_recv()
            pl.when(up != 0)(again[p].start)
            across_core(1, p).start()

    def hand_slot_3(pieces):
        for p in pieces:
            again[p].wait_recv()
            across_core(3, p).start()

    def where(condition, action, pieces):
        pl.when(condition)(lambda: action(pieces))

    every = range(PIECES)
    arrive(0)
    block(0, 0)
    where(prompt, hand_slot_2, (0, 1, 2))
    arrive(1)
    block(0, 1)
    where(prompt, hand_slot_2, (3, 4))
    where(odd == 1, hand_slot_1, every)
    arrive(2)
    block(0, 2)
    where(jnp.logical_and(late, even), hand_slot_2, every)

    one = 2 - odd
    for p in every:
        across_core(one, p).wait_recv()
    spread(weights[one], norm, groups, w_now)
    block(one, 0)
    where(even, hand_slot_1_upward, (0, 1, 2))
    where(blk == 1, hand_slot_2, (0, 1, 2))
    block(one, 1)
    where(even, hand_slot_1_upward, (3, 4))
    where(blk == 1, hand_slot_2, (3, 4))
    block(one, 2)

    two = 1 + odd
    for p in every:
        across_core(two, p).wait_recv()
    spread(weights[two], norm, groups, w_now)
    last_third = jnp.logical_or(blk == 1, blk == 2)
    block(two, 0)
    where(jnp.logical_and(odd == 1, prompt), hand_slot_3, every)
    block(two, 1)
    where(jnp.logical_and(even, blk != 2), hand_slot_3, every)
    block(two, 2)
    where(last_third, hand_slot_3, every)
    for p in every:
        across_core(3, p).wait_recv()
    spread(weights[3], norm, groups, w_ref)

    passed = [across_core(slot, p) for slot in (1, 2, 3) for p in every]
    for copy in sum(exchange, []) + upward + sideways + passed:
        copy.wait_send()

    @pl.when(odd == 0)
    def _():
        for copy in first:
            copy.wait_send()

    @pl.when(jnp.logical_and(odd == 0, up != 0))
    def _():
        for copy in again:
            copy.wait_send()

    @pl.when(to_first)
    def _():
        for copy in direct:
            copy.wait_send()


def compute_kernel(y_ref, c_ref, w_ref, x_ref, tm_ref, _, o_ref, f_ref, *scratch):
    for part in range(PACKED):
        at = pl.program_id(0) * PACKED + part
        shaped = scratch[part]
        shape_up(at, 3, c_ref, x_ref, tm_ref, shaped)
        pose(at, 3, y_ref, w_ref, shaped, f_ref.at[at])
        for c in range(CHUNK):
            for d in range(3):
                o_ref[part * CHUNK + c, d] = f_ref[at, d, pl.ds(ROW_GAP * c, 16), :].astype(BF16)


def per_device(n_blk, coefficients, transforms, basis, template, skin_weights):
    hbm = pl.BlockSpec(memory_space=pltpu.HBM)
    vmem = pl.BlockSpec(memory_space=pltpu.VMEM)
    shape = jax.ShapeDtypeStruct
    dma = pltpu.SemaphoreType.DMA
    gathered = pl.pallas_call(
        functools.partial(gather_kernel, n_blk),
        out_shape=[
            shape((CHUNKS, 3, CHUNK, 128), BF16),
            shape((R, K), BF16),
            shape((4, 128, VB), BF16),
            shape((STEPS, 3, K, VB), BF16),
            shape((STEPS, 3, VB), BF16),
            shape((CHUNKS, 3, STAGE_ROWS, 128), F32),
        ],
        in_specs=[hbm] * 5,
        out_specs=[vmem] * 6,
        scratch_shapes=[
            pltpu.VMEM((TURNS, 4, 12, 6, TURN), BF16),
            pltpu.VMEM((STEPS, J, VB), BF16),
            pltpu.VMEM((K, R), BF16),
            pltpu.VMEM((32, VB), F32),
            pltpu.VMEM((3, 128, TURN), F32),
            pltpu.VMEM((4, 128, VB), BF16),
            pltpu.VMEM((TURN // CHUNK, 2, 3, CHUNK, HALF), F32),
            pltpu.VMEM((CHUNKS, 2, 3, CHUNK, HALF), F32),
            dma((3, TURNS)), dma((3, TURNS)),
            dma((4, PIECES)), dma((4, PIECES)),
            dma((3, PIECES)), dma((3, PIECES)),
            dma((4 + TURNS,)),
        ],
        compiler_params=pltpu.CompilerParams(
            collective_id=0, has_side_effects=True, vmem_limit_bytes=GATHER_VMEM
        ),
        cost_estimate=pl.CostEstimate(flops=3 * 10**9, bytes_accessed=2 * 10**6, transcendentals=0),
        name="gather",
    )(*(
        pltpu.with_memory_space_constraint(a, pltpu.HBM)
        for a in (coefficients, transforms, jnp.transpose(basis, (1, 0, 2)), template, skin_weights)
    ))
    posed, _ = pl.pallas_call(
        compute_kernel,
        grid=(CHUNKS // PACKED,),
        out_shape=[shape((R, 3, 16, 128), BF16), gathered[5]],
        input_output_aliases={5: 1},
        in_specs=[vmem] * 6,
        out_specs=[pl.BlockSpec((PACKED * CHUNK, 3, 16, 128), lambda i: (i, 0, 0, 0)), vmem],
        scratch_shapes=[
            pltpu.VMEM((2, 3, CHUNK, HALF), F32),
        ] * PACKED,
        compiler_params=pltpu.CompilerParams(vmem_limit_bytes=COMPUTE_VMEM),
        cost_estimate=pl.CostEstimate(flops=10**9, bytes_accessed=10**7, transcendentals=0),
        name="compute",
    )(*gathered)
    return posed.reshape(R, 3, 4, STEPS, 128).transpose(0, 3, 1, 2, 4).reshape(R, STEPS, 3, VB)


def solution(mesh):
    both = ("blk", "batch")
    return jax.shard_map(
        functools.partial(per_device, mesh.shape["blk"]),
        mesh=mesh,
        in_specs=(P(None, both), P(None, "batch", "blk"), P(None, None, "blk"), P(None, "blk"), P(None, "blk")),
        out_specs=P(both, None, None, None),
        check_vma=False,
    )
```

```python
import functools

import jax
import jax.numpy as jnp
from jax import lax
from jax.experimental import pallas as pl
from jax.experimental.pallas import tpu as pltpu
from jax.sharding import PartitionSpec as P

MESH = pl.DeviceIdType.MESH
F32 = jnp.float32
BF16 = jnp.bfloat16
K, J, VB, R, STEPS = 120, 24, 512, 768, 4
CHUNK = 128
CHUNKS = R // CHUNK
HALF = VB // 2
PIECES = 5
ROW_GAP = 17
STAGE_ROWS = CHUNK * ROW_GAP + 8
TURNS = 3
TURN = R // TURNS
PACKED = 2
GATHER_VMEM = 20 * 2**20
COMPUTE_VMEM = 20 * 2**20


def spread(raw, norm, groups, out_ref):
    raw = raw.astype(F32)
    even = (raw / jnp.sum(raw, axis=0, keepdims=True)).astype(BF16).astype(F32)
    for g in range(4):
        norm[g * 8 : g * 8 + 6, :] = even[g * 6 : g * 6 + 6]
    rows = jnp.concatenate([norm[pl.ds(pl.multiple_of(g * 8, 8), 8), :] for g in groups], axis=0).astype(BF16)
    for e in range(4):
        out_ref[e, e * 32 : e * 32 + 32, :] = rows


def shape_up(at, s, c_ref, x_ref, tm_ref, shaped):
    rows = pl.ds(pl.multiple_of(at * CHUNK, CHUNK), CHUNK)
    for vt in range(2):
        span = slice(vt * HALF, (vt + 1) * HALF)
        for e in range(3):
            shaped[vt, e] = jnp.dot(
                c_ref[rows, :], x_ref[s, e, :, span], preferred_element_type=F32
            ) + tm_ref[s, e : e + 1, span].astype(F32)


def pose(at, s, y_ref, w_ref, shaped, staged):
    for vt in range(2):
        span = slice(vt * HALF, (vt + 1) * HALF)
        for d in range(3):
            poses = y_ref[at, d]
            total = jnp.dot(poses, w_ref[3, :, span], preferred_element_type=F32)
            for e in range(3):
                total = total + shaped[vt, e] * jnp.dot(poses, w_ref[e, :, span], preferred_element_type=F32)
            for h in range(2):
                place = (vt * 2 + h) * STEPS + s
                for c0 in range(0, CHUNK, 8):
                    staged[d, pl.ds(ROW_GAP * c0 + place, 8, stride=ROW_GAP), :] = total[
                        c0 : c0 + 8, h * 128 : (h + 1) * 128
                    ]


def gather_kernel(
    n_blk,
    coef_ref, tr_ref, bas_ref, tem_ref, wei_ref,
    y_ref, c_ref, w_ref, x_ref, tm_ref, f_ref,
    got, weights, coef, norm, zs, w_now, shaped, shaped_own,
    t_send, t_recv, b_send, b_recv, f_send, f_recv, local,
):
    blk = lax.axis_index("blk")
    me = lax.axis_index("batch")
    core = lax.rem(me, 2)
    hi = me // 2
    odd = lax.rem(blk, 2)
    sibling = hi * 2 + (1 - core)
    across = (1 - hi) * 2 + core
    diagonal = (1 - hi) * 2 + (1 - core)
    peers = (sibling, across, diagonal)
    groups = (me,) + peers
    up = lax.rem(blk + 2, n_blk)
    down = lax.rem(blk + n_blk - 2, n_blk)
    beside = blk + 1 - 2 * odd
    ahead = lax.rem(blk + 1, n_blk)
    behind = lax.rem(blk + n_blk - 1, n_blk)
    to_first = ahead == 0
    from_last = blk == 0
    half = pl.ds(pl.multiple_of(core * HALF, HALF), HALF)

    own = [
        pltpu.make_async_copy(coef_ref, coef, local.at[0]),
        pltpu.make_async_copy(bas_ref, x_ref.at[0], local.at[1]),
        pltpu.make_async_copy(wei_ref, weights.at[0], local.at[2]),
        pltpu.make_async_copy(tem_ref, tm_ref.at[0], local.at[3]),
    ]

    def turn_of(device, turn):
        return tr_ref.at[:, :, pl.ds(pl.multiple_of(device * R + turn * TURN, TURN), TURN)]

    kept = [pltpu.make_async_copy(turn_of(me, turn), got.at[turn, 0], local.at[4 + turn]) for turn in range(TURNS)]
    for copy in own + kept:
        copy.start()

    barrier = pltpu.get_barrier_semaphore()
    for target in ((blk, sibling), (blk, across), (blk, diagonal), (beside, across), (down, me)):
        pl.semaphore_signal(barrier, inc=1, device_id=target, device_id_type=MESH)
    pl.when(from_last)(
        lambda: pl.semaphore_signal(barrier, inc=1, device_id=(behind, across), device_id_type=MESH)
    )
    pl.semaphore_wait(barrier, 5 + (blk + 1) // n_blk)

    def remote(src, dst, send, recv, target):
        return pltpu.make_async_remote_copy(
            src_ref=src, dst_ref=dst, send_sem=send, recv_sem=recv, device_id=target, device_id_type=MESH
        )

    def slot_parts(slot, span):
        return [weights.at[slot, :, span], tm_ref.at[slot, :, span]] + [
            x_ref.at[slot, e, :, span] for e in range(3)
        ]

    def own_parts(span):
        return [wei_ref.at[:, span], tem_ref.at[:, span]] + [bas_ref.at[e, :, span] for e in range(3)]

    first = [
        remote(s, d, b_send.at[0, p], b_recv.at[1, p], (beside, across))
        for p, (s, d) in enumerate(zip(own_parts(half), slot_parts(1, half)))
    ]
    upward = [
        remote(s, d, b_send.at[1, p], b_recv.at[2, p], (up, me))
        for p, (s, d) in enumerate(zip(own_parts(half), slot_parts(2, half)))
    ]
    third = 3 - 2 * odd
    sideways = [
        remote(s, d, b_send.at[2, p], b_recv.at[third, p], (beside, across))
        for p, (s, d) in enumerate(zip(slot_parts(2, half), slot_parts(third, half)))
    ]
    again = [
        remote(s, d, b_send.at[3, p], b_recv.at[3, p], (up, me))
        for p, (s, d) in enumerate(zip(slot_parts(1, half), slot_parts(3, half)))
    ]
    direct = [
        remote(s, d, b_send.at[0, p], b_recv.at[3, p], (ahead, across))
        for p, (s, d) in enumerate(zip(slot_parts(2, half), slot_parts(3, half)))
    ]

    def across_core(slot, p):
        part = slot_parts(slot, half)[p]
        return remote(part, part, f_send.at[slot - 1, p], f_recv.at[slot - 1, p], (blk, sibling))

    exchange = [
        [
            remote(turn_of(peer, turn), got.at[turn, r + 1], t_send.at[r, turn], t_recv.at[r, turn], (blk, peer))
            for r, peer in enumerate(peers)
        ]
        for turn in range(TURNS)
    ]
    for turn in range(TURNS):
        for copy in exchange[turn]:
            copy.start()
    for copy in upward:
        copy.start()

    @pl.when(odd == 0)
    def _():
        for copy in first:
            copy.start()

    zs[...] = jnp.zeros_like(zs)
    norm[...] = jnp.zeros_like(norm)
    w_now[...] = jnp.zeros_like(w_now)
    w_ref[...] = jnp.zeros_like(w_ref)
    own[0].wait()
    for at in range(CHUNKS):
        part = slice(at * CHUNK, (at + 1) * CHUNK)
        c_ref[part, :] = coef[:, part].astype(F32).T.astype(BF16)
    for k in (1, 2, 3):
        own[k].wait()
    spread(weights[0], norm, groups, w_now)

    parts = TURN // CHUNK
    for at in range(CHUNKS):
        shape_up(at, 0, c_ref, x_ref, tm_ref, shaped_own.at[at])

    def arrive(turn):
        kept[turn].wait()
        for copy in exchange[turn]:
            copy.wait_recv()
        for m in range(12):
            for r in range(4):
                row = (m % 4) * 32 + r * 8
                zs[m // 4, row : row + 6, :] = got[turn, r, m].astype(F32)
        for part in range(parts):
            for d in range(3):
                y_ref[turn * parts + part, d] = zs[d, :, part * CHUNK : (part + 1) * CHUNK].T.astype(BF16)

    def block(s, turn):
        for part in range(parts):
            at = turn * parts + part
            if turn_is_own(s):
                mine = shaped_own.at[at]
            else:
                mine = shaped.at[part]
                shape_up(at, s, c_ref, x_ref, tm_ref, mine)
            pose(at, s, y_ref, w_now, mine, f_ref.at[at])

    def turn_is_own(s):
        return isinstance(s, int)

    even = odd == 0
    late = blk < 2
    prompt = jnp.logical_not(late)

    def hand_slot_2(pieces):
        @pl.when(to_first)
        def _():
            for p in pieces:
                upward[p].wait_recv()
                direct[p].start()
            for p in pieces:
                sideways[p].start()
                across_core(2, p).start()

        @pl.when(jnp.logical_not(to_first))
        def _():
            for p in pieces:
                upward[p].wait_recv()
                sideways[p].start()
                across_core(2, p).start()

    def hand_slot_1(pieces):
        for p in pieces:
            first[p].wait_recv()
            across_core(1, p).start()

    def hand_slot_1_upward(pieces):
        for p in pieces:
            first[p].wait_recv()
            pl.when(up != 0)(again[p].start)
            across_core(1, p).start()

    def hand_slot_3(pieces):
        for p in pieces:
            again[p].wait_recv()
            across_core(3, p).start()

    def where(condition, action, pieces):
        pl.when(condition)(lambda: action(pieces))

    every = range(PIECES)
    arrive(0)
    block(0, 0)
    where(prompt, hand_slot_2, (0, 1, 2))
    arrive(1)
    block(0, 1)
    where(prompt, hand_slot_2, (3, 4))
    where(odd == 1, hand_slot_1, every)
    arrive(2)
    block(0, 2)
    where(jnp.logical_and(late, even), hand_slot_2, every)

    one = 2 - odd
    for p in every:
        across_core(one, p).wait_recv()
    spread(weights[one], norm, groups, w_now)
    where(from_last, hand_slot_1_upward, (0, 1, 2))
    block(one, 0)
    where(jnp.logical_and(even, prompt), hand_slot_1_upward, (0, 1, 2))
    where(from_last, hand_slot_1_upward, (3,))
    where(blk == 1, hand_slot_2, (0, 1, 2))
    block(one, 1)
    where(jnp.logical_and(even, prompt), hand_slot_1_upward, (3, 4))
    where(from_last, hand_slot_1_upward, (4,))
    where(blk == 1, hand_slot_2, (3, 4))
    block(one, 2)

    two = 1 + odd
    for p in every:
        across_core(two, p).wait_recv()
    spread(weights[two], norm, groups, w_now)
    last_third = jnp.logical_or(blk == 1, blk == 2)
    block(two, 0)
    where(jnp.logical_and(odd == 1, prompt), hand_slot_3, every)
    block(two, 1)
    where(jnp.logical_and(even, blk != 2), hand_slot_3, every)
    block(two, 2)
    where(last_third, hand_slot_3, every)
    for p in every:
        across_core(3, p).wait_recv()
    spread(weights[3], norm, groups, w_ref)

    passed = [across_core(slot, p) for slot in (1, 2, 3) for p in every]
    for copy in sum(exchange, []) + upward + sideways + passed:
        copy.wait_send()

    @pl.when(odd == 0)
    def _():
        for copy in first:
            copy.wait_send()

    @pl.when(jnp.logical_and(odd == 0, up != 0))
    def _():
        for copy in again:
            copy.wait_send()

    @pl.when(to_first)
    def _():
        for copy in direct:
            copy.wait_send()


def compute_kernel(y_ref, c_ref, w_ref, x_ref, tm_ref, _, o_ref, f_ref, *scratch):
    for part in range(PACKED):
        at = pl.program_id(0) * PACKED + part
        shaped = scratch[part]
        shape_up(at, 3, c_ref, x_ref, tm_ref, shaped)
        pose(at, 3, y_ref, w_ref, shaped, f_ref.at[at])
        for c in range(CHUNK):
            for d in range(3):
                o_ref[part * CHUNK + c, d] = f_ref[at, d, pl.ds(ROW_GAP * c, 16), :].astype(BF16)


def per_device(n_blk, coefficients, transforms, basis, template, skin_weights):
    hbm = pl.BlockSpec(memory_space=pltpu.HBM)
    vmem = pl.BlockSpec(memory_space=pltpu.VMEM)
    shape = jax.ShapeDtypeStruct
    dma = pltpu.SemaphoreType.DMA
    gathered = pl.pallas_call(
        functools.partial(gather_kernel, n_blk),
        out_shape=[
            shape((CHUNKS, 3, CHUNK, 128), BF16),
            shape((R, K), BF16),
            shape((4, 128, VB), BF16),
            shape((STEPS, 3, K, VB), BF16),
            shape((STEPS, 3, VB), BF16),
            shape((CHUNKS, 3, STAGE_ROWS, 128), F32),
        ],
        in_specs=[hbm] * 5,
        out_specs=[vmem] * 6,
        scratch_shapes=[
            pltpu.VMEM((TURNS, 4, 12, 6, TURN), BF16),
            pltpu.VMEM((STEPS, J, VB), BF16),
            pltpu.VMEM((K, R), BF16),
            pltpu.VMEM((32, VB), F32),
            pltpu.VMEM((3, 128, TURN), F32),
            pltpu.VMEM((4, 128, VB), BF16),
            pltpu.VMEM((TURN // CHUNK, 2, 3, CHUNK, HALF), F32),
            pltpu.VMEM((CHUNKS, 2, 3, CHUNK, HALF), F32),
            dma((3, TURNS)), dma((3, TURNS)),
            dma((4, PIECES)), dma((4, PIECES)),
            dma((3, PIECES)), dma((3, PIECES)),
            dma((4 + TURNS,)),
        ],
        compiler_params=pltpu.CompilerParams(
            collective_id=0, has_side_effects=True, vmem_limit_bytes=GATHER_VMEM
        ),
        cost_estimate=pl.CostEstimate(flops=3 * 10**9, bytes_accessed=2 * 10**6, transcendentals=0),
        name="gather",
    )(*(
        pltpu.with_memory_space_constraint(a, pltpu.HBM)
        for a in (coefficients, transforms, jnp.transpose(basis, (1, 0, 2)), template, skin_weights)
    ))
    posed, _ = pl.pallas_call(
        compute_kernel,
        grid=(CHUNKS // PACKED,),
        out_shape=[shape((R, 3, 16, 128), BF16), gathered[5]],
        input_output_aliases={5: 1},
        in_specs=[vmem] * 6,
        out_specs=[pl.BlockSpec((PACKED * CHUNK, 3, 16, 128), lambda i: (i, 0, 0, 0)), vmem],
        scratch_shapes=[
            pltpu.VMEM((2, 3, CHUNK, HALF), F32),
        ] * PACKED,
        compiler_params=pltpu.CompilerParams(vmem_limit_bytes=COMPUTE_VMEM),
        cost_estimate=pl.CostEstimate(flops=10**9, bytes_accessed=10**7, transcendentals=0),
        name="compute",
    )(*gathered)
    return posed.reshape(R, 3, 4, STEPS, 128).transpose(0, 3, 1, 2, 4).reshape(R, STEPS, 3, VB)


def solution(mesh):
    both = ("blk", "batch")
    return jax.shard_map(
        functools.partial(per_device, mesh.shape["blk"]),
        mesh=mesh,
        in_specs=(P(None, both), P(None, "batch", "blk"), P(None, None, "blk"), P(None, "blk"), P(None, "blk")),
        out_specs=P(both, None, None, None),
        check_vma=False,
    )
```
